256 devices in a mesh: strip: 32 (over z, x), col: 8 (over y, core).
Axes of the slice: x: 4, y: 4, z: 8, core: 2. Of those that a mesh axis runs over, the one named last changes fastest.
Arguments:
- residuals: float32 [64, 64, 2560], P('strip'), may hold values from -6 to 6
- corr_rows: float32 [64], replicated, may hold values from 0.5 to 2
- corr_cols: float32 [2560], replicated, may hold values from 0.5 to 2
- row_anchor: int32 [64], replicated, may hold values from 0 to 448
- col_anchor: int32 [64], replicated, may hold values from 0 to 17920
- valid_first: int32 [64], replicated, may hold values from 0 to 15
- valid_end: int32 [64], replicated, may hold values from 49 to 64
- facet_of_slot: int32 [64], replicated, may hold values from 0 to 63, each once
Outputs:
- stitched: float32 [512, 20480], P('strip', 'col')
- column_power: float32 [20480], P('col')
The draws below stay inside these ranges and needn't reach their ends.
Inputs may be any that keep to these rules, and one draw needn't show every extreme that they name: facet_of_slot names each of the 64 facets exactly once.
All inputs are finite; a program needn't handle non-finite values.
Results may differ from the reference program's by a relative error of at most 0.0003.
Values sent between devices are 32-bit elements; how exact they have to be, the bound alone decides.
A program may use at most 64 MiB of HBM per device.

```python
import math
import jax
import jax.numpy as jnp
from jax import lax

FW = 2560
FH = 64
FACETS = 64
MH = 512
MW = 20480


def with_ends(array, stream_key, low, largest):
    place = [jax.random.randint(jax.random.fold_in(stream_key, axis), (), 0, length) for axis, length in enumerate(array.shape)]
    longest = array.shape.index(max(array.shape))
    neighbour = place[:longest] + [(place[longest] + 1) % array.shape[longest]] + place[longest + 1:]
    return array.at[tuple(place)].set(low).at[tuple(neighbour)].set(largest)


def level_of(rng, shape, shards, smallest, high):
    loudness, own = 1.0, jax.random.fold_in(rng, 6)
    for dim, parts in shards:
        steps = jnp.exp(jax.random.uniform(jax.random.fold_in(own, dim), (parts,), jnp.float32, smallest / len(shards), high / len(shards)))
        loudness = loudness * jnp.repeat(steps, shape[dim] // parts).reshape([-1 if axis == dim else 1 for axis in range(len(shape))])
    return loudness


def scatter_about(rng, extent, deviation, most, split=(), dtype=jnp.bfloat16):
    entries = jax.random.normal(rng, extent, jnp.float32) * deviation
    if len(split) > 0:
        entries = level_of(rng, extent, split, -0.22, 0.18) * entries
    return jnp.clip(entries, min=-most, max=most).astype(dtype)


def setup_inputs(seed: int = 0) -> dict:
    keys = jax.random.split(jax.random.key(seed), 9)
    residuals = scatter_about(keys[0], (FACETS, FH, FW), 1.0, 6.0, ((0, 32),), jnp.float32)
    corr_rows = jnp.clip(jnp.exp(jax.random.uniform(keys[1], (FH,), jnp.float32, math.log(0.5), math.log(2.0))), 0.5, 2.0)
    corr_cols = jnp.clip(jnp.exp(jax.random.uniform(keys[2], (FW,), jnp.float32, math.log(0.5), math.log(2.0))), 0.5, 2.0)
    row_anchor = with_ends(jax.random.randint(keys[3], (FACETS,), 0, MH - FH + 1), jax.random.fold_in(keys[3], 1), 0, MH - FH).astype(jnp.int32)
    col_anchor = with_ends(jax.random.randint(keys[4], (FACETS,), 0, MW - FW + 1), jax.random.fold_in(keys[4], 1), 0, MW - FW).astype(jnp.int32)
    valid_first = with_ends(jax.random.randint(keys[5], (FACETS,), 0, FH // 4), jax.random.fold_in(keys[5], 1), 0, (FH // 4) - 1).astype(jnp.int32)
    valid_end = with_ends(jax.random.randint(keys[6], (FACETS,), 3 * FH // 4 + 1, FH + 1), jax.random.fold_in(keys[6], 1), 3 * FH // 4 + 1, FH).astype(jnp.int32)
    facet_of_slot = jax.random.permutation(keys[7], FACETS).astype(jnp.int32)
    return dict(residuals=residuals, corr_rows=corr_rows, corr_cols=corr_cols, row_anchor=row_anchor, col_anchor=col_anchor, valid_first=valid_first, valid_end=valid_end, facet_of_slot=facet_of_slot)


def tapers(count):
    position = (jnp.arange(count).astype(jnp.float32) + 0.5) / count
    return jnp.sin(jnp.pi * position) ** 2


def reference(residuals, corr_rows, corr_cols, row_anchor, col_anchor, valid_first, valid_end, facet_of_slot):
    facet_rows = residuals.shape[1]
    facet_cols = residuals.shape[2]
    row_index = jnp.arange(facet_rows).astype(jnp.int32)
    row_taper = tapers(facet_rows)
    col_taper = tapers(facet_cols)
    correction = corr_rows[:, None] * corr_cols[None, :]

    def accumulate(running, position):
        numerator, denominator = running
        facet_id = facet_of_slot[position]
        row_start = row_anchor[facet_id]
        col_start = col_anchor[facet_id]
        inside = (row_index >= valid_first[facet_id]) & (row_index < valid_end[facet_id])
        row_weight = jnp.where(inside, row_taper, 0.0)
        weight = row_weight[:, None] * col_taper[None, :]
        weighted = weight * correction * residuals[position]
        old_num = lax.dynamic_slice(numerator, (row_start, col_start), (facet_rows, facet_cols))
        numerator = lax.dynamic_update_slice(numerator, old_num + weighted, (row_start, col_start))
        old_den = lax.dynamic_slice(denominator, (row_start, col_start), (facet_rows, facet_cols))
        denominator = lax.dynamic_update_slice(denominator, old_den + weight, (row_start, col_start))
        return (numerator, denominator), None

    blank = jnp.zeros((MH, MW), jnp.float32)
    (numerator, denominator), _ = lax.scan(accumulate, (blank, blank), jnp.arange(FACETS).astype(jnp.int32))
    stitched = numerator / jnp.maximum(denominator, 0.5)
    column_power = jnp.mean(stitched * stitched, axis=0)
    return (stitched, column_power)
```

```python
import jax
import jax.numpy as jnp
from jax import lax
from jax.experimental import pallas as pl
from jax.experimental.pallas import tpu as pltpu
from jax.sharding import PartitionSpec as P


MESH = pl.DeviceIdType.MESH
FH, FW, SLOTS, ROWS, QUARTER, LANES = 64, 2560, 64, 16, 640, 128
STRIPS, COLS, ZS, XS = 32, 8, 8, 4


def squared_sine(position, count):
    return jnp.sin(jnp.pi * ((position.astype(jnp.float32) + 0.5) / count)) ** 2


def parts_of(value):
    first = value.astype(jnp.bfloat16)
    rest = value - first.astype(jnp.float32)
    second = rest.astype(jnp.bfloat16)
    third = (rest - second.astype(jnp.float32)).astype(jnp.bfloat16)
    return first, second, third


def binned(one_hot, upper, value):
    placed = jnp.concatenate([jnp.where(upper, value, 0.0), jnp.where(upper, 0.0, value)], axis=0)
    total = None
    for part in parts_of(placed):
        product = jnp.dot(one_hot, part, preferred_element_type=jnp.float32)
        total = product if total is None else total + product
    return total


def wait_for(ref, sem):
    pltpu.make_async_copy(ref, ref, sem).wait()


def kernel(
    res_hbm, crow, ccol, fos_v, ra_v, ca_v, vf_v, ve_v, fos_s, ra_s, ca_s, vf_s, ve_s,
    out, power,
    data, rowfac, colfac, turned, send1, recv1, tile, psum, pgot, psend, pall,
    load_sem, s1, r1, s2, r2, s3, r3, s4, r4,
):
    strip = lax.axis_index("strip")
    col = lax.axis_index("col")
    z, x = strip // XS, strip % XS
    y, core = col // 2, col % 2

    load = pltpu.make_async_copy(res_hbm, data, load_sem)
    load.start()

    barrier = pltpu.get_barrier_semaphore()

    def greet(peer_strip, peer_col):
        pl.semaphore_signal(barrier, inc=1, device_id=(peer_strip, peer_col), device_id_type=MESH)

    @pl.loop(1, STRIPS)
    def _(step):
        greet((strip + step) % STRIPS, col)

    @pl.loop(0, ZS * (COLS - 1))
    def _(step):
        greet(((z + step // (COLS - 1)) % ZS) * XS + x, (col + 1 + step % (COLS - 1)) % COLS)

    @pl.loop(1, XS)
    def _(step):
        greet(z * XS + (x + step) % XS, 2 * y + 1 - core)

    diagonal = lax.broadcasted_iota(jnp.int32, (SLOTS, SLOTS), 0) == lax.broadcasted_iota(jnp.int32, (SLOTS, SLOTS), 1)

    def upright(row):
        return jnp.sum(jnp.where(diagonal, row, 0.0), axis=1, keepdims=True)

    row_index = lax.broadcasted_iota(jnp.int32, (FH, LANES), 0)
    row_base = squared_sine(row_index, FH) * upright(crow[...])
    colfac[...] = squared_sine(lax.broadcasted_iota(jnp.int32, (8, FW), 1), FW) * ccol[...]
    facets = []
    for i in range(2):
        facet = fos_s[2 * strip + i]
        inside = (row_index >= vf_s[facet]) & (row_index < ve_s[facet])
        rowfac[i] = jnp.where(inside, row_base, 0.0)
        facets.append((ra_s[facet], ca_s[facet]))
    load.wait()

    sub = lax.broadcasted_iota(jnp.int32, (8, LANES), 0)
    lane = lax.broadcasted_iota(jnp.int32, (8, LANES), 1)
    for i in range(2):
        row_anchor, col_anchor = facets[i]
        first_row = lax.rem(8 * core + 448 - row_anchor, FH)
        first_col = lax.rem(QUARTER * y + 17920 - col_anchor, FW)
        group, row_off = lax.div(first_row, 8), lax.rem(first_row, 8)
        column, col_off = lax.div(first_col, LANES), lax.rem(first_col, LANES)
        row_roll, col_roll = lax.rem(8 - row_off, 8), lax.rem(LANES - col_off, LANES)
        in_first_row, in_first_col = sub < 8 - row_off, lane < LANES - col_off
        group, column = jnp.full((8, LANES), group), jnp.full((8, LANES), column)
        for k in range(8):
            row_factor = rowfac[i, 8 * k : 8 * k + 8, :]
            tiles = []
            for n in range(FW // LANES):
                part = pl.ds(LANES * n, LANES)
                tiles.append(data[i, pl.ds(8 * k, 8), part] * (row_factor * colfac[:, part]))
            for bit, count in ((16, 20), (8, 13), (4, 9), (2, 7), (1, 6)):
                moved = (column & bit) != 0
                tiles = [jnp.where(moved, tiles[(n + bit) % len(tiles)], tiles[n]) for n in range(count)]
            tiles = [pltpu.roll(tile_n, col_roll, 1) for tile_n in tiles]
            for n in range(5):
                turned[k, :, LANES * n : LANES * (n + 1)] = jnp.where(in_first_col, tiles[n], tiles[n + 1])
        for n in range(5):
            part = pl.ds(LANES * n, LANES)
            rows = [turned[k, :, part] for k in range(8)]
            for bit in (4, 2, 1):
                moved = (group & bit) != 0
                rows = [jnp.where(moved, rows[(k + bit) % 8], rows[k]) for k in range(8)]
            rows = [pltpu.roll(row_k, row_roll, 0) for row_k in rows]
            for xq in range(XS):
                send1[xq, :, i, part] = jnp.where(in_first_row, rows[2 * xq], rows[2 * xq + 1])

    pl.semaphore_wait(barrier, 90)

    @pl.loop(1, STRIPS)
    def _(step):
        peer = (strip + step) % STRIPS
        pltpu.make_async_remote_copy(
            src_ref=send1.at[peer % XS, peer // XS], dst_ref=recv1.at[strip], send_sem=s1, recv_sem=r1,
            device_id=(peer, col), device_id_type=MESH,
        ).start()

    pltpu.make_async_copy(send1.at[x, z], recv1.at[strip], r1).start()

    m = 16 * x + 8 * core + z
    facet_of = upright(fos_v[...].astype(jnp.float32)).astype(jnp.int32)
    chosen = facet_of == lax.broadcasted_iota(jnp.int32, (SLOTS, SLOTS), 1)

    def by_slot(row):
        return jnp.sum(jnp.where(chosen, row.astype(jnp.float32), 0.0), axis=1, keepdims=True).astype(jnp.int32)

    ra, ca, vf, ve = (by_slot(ref[...]) for ref in (ra_v, ca_v, vf_v, ve_v))
    block = (ra >> 6) + (m < (ra & 63)).astype(jnp.int32)
    facet_row = (m - ra) & 63
    row_weight = jnp.where((facet_row >= vf) & (facet_row < ve), squared_sine(facet_row, FH), 0.0)
    column_group = sum((ca >= FW * k).astype(jnp.int32) for k in range(1, COLS))
    first_class = ca - FW * column_group
    class_index = QUARTER * y + lax.broadcasted_iota(jnp.int32, (SLOTS, QUARTER), 1)
    upper = class_index >= first_class
    facet_col = class_index - first_class + jnp.where(upper, 0, FW)
    weight = row_weight * squared_sine(facet_col, FW)
    wide_lane = lax.broadcasted_iota(jnp.int32, (SLOTS, 2 * SLOTS), 1)
    wide_sub = lax.broadcasted_iota(jnp.int32, (SLOTS, 2 * SLOTS), 0)
    low_bin = (8 * block + column_group).astype(jnp.float32)
    bin_row = jnp.sum(jnp.where((wide_lane & 63) == wide_sub, low_bin, 0.0), axis=0, keepdims=True)
    bin_row = bin_row.astype(jnp.int32) + (wide_lane[:1] >> 6)
    one_hot = (wide_sub == bin_row).astype(jnp.float32).astype(jnp.bfloat16)
    scale = 1.0 / jnp.maximum(binned(one_hot, upper, weight), 0.5)

    wait_for(recv1, r1)
    stitched = binned(one_hot, upper, recv1[...].reshape(SLOTS, QUARTER)) * scale
    tile[...] = stitched
    squares = stitched * stitched
    sums = squares[0:8]
    for q in range(1, 8):
        sums = sums + squares[8 * q : 8 * q + 8]
    psum[0] = sums[0:4]
    psum[1] = sums[4:8]

    place = 2 * x + core

    @pl.loop(1, 8)
    def _(step):
        peer = (place + step) % 8
        pltpu.make_async_remote_copy(
            src_ref=psum.at[peer % 2], dst_ref=pgot.at[place], send_sem=s3, recv_sem=r3,
            device_id=(z * XS + peer // 2, 2 * y + peer % 2), device_id_type=MESH,
        ).start()

    pltpu.make_async_copy(psum.at[core], pgot.at[place], r3).start()

    own_bin = 8 * z + col
    out_row = 8 * core + z
    out_cols = pl.ds(pl.multiple_of(QUARTER * y, LANES), QUARTER)

    @pl.loop(1, 64)
    def _(step):
        peer = (own_bin + step) % 64
        pltpu.make_async_remote_copy(
            src_ref=tile.at[peer], dst_ref=out.at[out_row, out_cols], send_sem=s2, recv_sem=r2,
            device_id=((peer // 8) * XS + x, peer % 8), device_id_type=MESH,
        ).start()

    pltpu.make_async_copy(tile.at[own_bin], out.at[out_row, out_cols], r2).start()

    wait_for(pgot, r3)
    total = pgot[0]
    for k in range(1, 8):
        total = total + pgot[k]
    psend[...] = total

    @pl.loop(0, 32)
    def _(step):
        peer_z = (z + step // 4) % ZS
        peer_col = 4 * core + step % 4
        own = (step < 4) & (peer_col == col)

        @pl.when(own)
        def _():
            pltpu.make_async_copy(psend.at[step % 4], pall.at[z, out_cols], r4).start()

        @pl.when(jnp.logical_not(own))
        def _():
            pltpu.make_async_remote_copy(
                src_ref=psend.at[step % 4], dst_ref=pall.at[z, out_cols], send_sem=s4, recv_sem=r4,
                device_id=(peer_z * XS + x, peer_col), device_id_type=MESH,
            ).start()

    wait_for(pall, r4)
    power[...] = jnp.sum(pall[...], axis=0, keepdims=True) / (FH * 8)
    wait_for(out, r2)

    wait_for(recv1.at[pl.ds(0, STRIPS - 1)], s1)
    wait_for(pgot.at[pl.ds(0, 7)], s3)

    @pl.loop(1, 64)
    def _(step):
        wait_for(tile.at[0], s2)

    @pl.loop(0, 32)
    def _(step):
        @pl.when(jnp.logical_not((step < 4) & (4 * core + step % 4 == col)))
        def _():
            wait_for(psend.at[0], s4)


def body(residuals, corr_rows, corr_cols, row_anchor, col_anchor, valid_first, valid_end, facet_of_slot):
    ints = (facet_of_slot, row_anchor, col_anchor, valid_first, valid_end)
    vmem = pl.BlockSpec(memory_space=pltpu.VMEM)
    smem = pl.BlockSpec(memory_space=pltpu.SMEM)
    f32 = jnp.float32
    dma = pltpu.SemaphoreType.DMA
    stitched, power = pl.pallas_call(
        kernel,
        out_shape=(jax.ShapeDtypeStruct((ROWS, FW), f32), jax.ShapeDtypeStruct((1, FW), f32)),
        in_specs=[pl.BlockSpec(memory_space=pl.ANY)] + [vmem] * 7 + [smem] * 5,
        out_specs=(vmem, vmem),
        scratch_shapes=[
            pltpu.VMEM((2, FH, FW), f32),
            pltpu.VMEM((2, FH, LANES), f32),
            pltpu.VMEM((8, FW), f32),
            pltpu.VMEM((8, 8, QUARTER), f32),
            pltpu.VMEM((XS, ZS, 2, QUARTER), f32),
            pltpu.VMEM((STRIPS, 2, QUARTER), f32),
            pltpu.VMEM((64, QUARTER), f32),
            pltpu.VMEM((2, 4, QUARTER), f32),
            pltpu.VMEM((8, 4, QUARTER), f32),
            pltpu.VMEM((4, QUARTER), f32),
            pltpu.VMEM((ZS, FW), f32),
        ]
        + [dma] * 9,
        compiler_params=pltpu.CompilerParams(collective_id=0, has_side_effects=True),
        name="restitch",
    )(
        residuals, corr_rows.reshape(1, FH), corr_cols.reshape(1, FW),
        *(a.reshape(1, SLOTS) for a in ints), *ints,
    )
    return stitched, power.reshape(FW)


def solution(mesh):
    in_specs = (P("strip", None, None), P(), P(), P(), P(), P(), P(), P())
    out_specs = (P("strip", "col"), P("col"))
    return jax.shard_map(body, mesh=mesh, in_specs=in_specs, out_specs=out_specs, check_vma=False)
```

```python
import jax
import jax.numpy as jnp
from jax import lax
from jax.experimental import pallas as pl
from jax.experimental.pallas import tpu as pltpu
from jax.sharding import PartitionSpec as P


MESH = pl.DeviceIdType.MESH
FH, FW, SLOTS, ROWS, QUARTER, LANES = 64, 2560, 64, 16, 640, 128
STRIPS, COLS, ZS, XS, TILES = 32, 8, 8, 4, 20
FAR_FIRST = (4, 3, 5, 2, 6, 1, 7, 0)


def squared_sine(position, count):
    return jnp.sin(jnp.pi * ((position.astype(jnp.float32) + 0.5) / count)) ** 2


def parts_of(value):
    first = value.astype(jnp.bfloat16)
    rest = value - first.astype(jnp.float32)
    second = rest.astype(jnp.bfloat16)
    third = (rest - second.astype(jnp.float32)).astype(jnp.bfloat16)
    return first, second, third


def binned(one_hot, upper, value):
    placed = jnp.concatenate([jnp.where(upper, value, 0.0), jnp.where(upper, 0.0, value)], axis=0)
    total = None
    for part in parts_of(placed):
        product = jnp.dot(one_hot, part, preferred_element_type=jnp.float32)
        total = product if total is None else total + product
    return total


def wait_for(ref, sem):
    pltpu.make_async_copy(ref, ref, sem).wait()


def kernel(
    res_hbm, crow_hbm, ccol_hbm, rows_hbm, ints_hbm,
    land, pall,
    data, crow, ccol, ints_v, ints_s, rowfac, colfac, turned, send1, recv1, tile, psum, pgot, psend,
    load_sems, s1, r1, s2, r2, s3, r3, s4, r4,
):
    strip = lax.axis_index("strip")
    col = lax.axis_index("col")
    z, x = strip >> 2, strip & 3
    y, core = col >> 1, col & 1

    def plane():
        for dz in FAR_FIRST:
            for dx in (2, 1, 3, 0):
                if dz or dx:
                    yield ((z + dz) & 7), ((x + dx) & 3)

    barrier = pltpu.get_barrier_semaphore()
    for pz, px in plane():
        pl.semaphore_signal(barrier, inc=1, device_id=((pz << 2) + px, col), device_id_type=MESH)
    for step in range(1, COLS):
        pl.semaphore_signal(barrier, inc=1, device_id=(strip, (col + step) & 7), device_id_type=MESH)

    loads = [pltpu.make_async_copy(h, v, load_sems.at[n]) for n, (h, v) in enumerate(
        [(ints_hbm[k], ints_s.at[k]) for k in range(5)] + [(crow_hbm, crow), (ccol_hbm, ccol)]
        + [(rows_hbm[k], ints_v.at[k]) for k in range(5)] + [(res_hbm, data)]
    )]
    for load in loads:
        load.start()

    diagonal = lax.broadcasted_iota(jnp.int32, (SLOTS, SLOTS), 0) == lax.broadcasted_iota(jnp.int32, (SLOTS, SLOTS), 1)

    def upright(row):
        return jnp.sum(jnp.where(diagonal, row, 0.0), axis=1, keepdims=True)

    row_index = lax.broadcasted_iota(jnp.int32, (FH, LANES), 0)
    row_base = squared_sine(row_index, FH)
    col_base = squared_sine(lax.broadcasted_iota(jnp.int32, (8, FW), 1), FW)
    for load in loads[:-1]:
        load.wait()
    row_base = row_base * upright(crow[...])
    for n in range(TILES):
        part = slice(LANES * n, LANES * (n + 1))
        colfac[:, part] = col_base[:, part] * ccol[n : n + 1, :]
    facets = []
    for i in range(2):
        facet = ints_s[0, 2 * strip + i]
        inside = (row_index >= ints_s[3, facet]) & (row_index < ints_s[4, facet])
        rowfac[i] = jnp.where(inside, row_base, 0.0)
        facets.append((ints_s[1, facet], ints_s[2, facet]))
    loads[-1].wait()

    sub = lax.broadcasted_iota(jnp.int32, (8, LANES), 0)
    lane = lax.broadcasted_iota(jnp.int32, (8, LANES), 1)
    for i in range(2):
        row_anchor, col_anchor = facets[i]
        first_row = (8 * core + 448 - row_anchor) & 63
        first_col = lax.rem(QUARTER * y + 17920 - col_anchor, FW)
        group, row_off = first_row >> 3, first_row & 7
        column, col_off = first_col >> 7, first_col & 127
        row_roll, col_roll = (8 - row_off) & 7, (LANES - col_off) & 127
        in_first_row, in_first_col = sub < 8 - row_off, lane < LANES - col_off
        group, column = jnp.full((8, LANES), group), jnp.full((8, LANES), column)
        for k in range(8):
            row_factor = rowfac[i, 8 * k : 8 * k + 8, :]
            tiles = []
            for n in range(TILES):
                part = pl.ds(LANES * n, LANES)
                tiles.append(data[i, pl.ds(8 * k, 8), part] * (row_factor * colfac[:, part]))
            for bit, count in ((16, 20), (8, 13), (4, 9), (2, 7), (1, 6)):
                moved = (column & bit) != 0
                tiles = [jnp.where(moved, tiles[(n + bit) % len(tiles)], tiles[n]) for n in range(count)]
            tiles = [pltpu.roll(tile_n, col_roll, 1) for tile_n in tiles]
            for n in range(5):
                turned[k, :, LANES * n : LANES * (n + 1)] = jnp.where(in_first_col, tiles[n], tiles[n + 1])
        for n in range(5):
            part = pl.ds(LANES * n, LANES)
            rows = [turned[k, :, part] for k in range(8)]
            for bit in (4, 2, 1):
                moved = (group & bit) != 0
                rows = [jnp.where(moved, rows[(k + bit) % 8], rows[k]) for k in range(8)]
            rows = [pltpu.roll(row_k, row_roll, 0) for row_k in rows]
            for xq in range(XS):
                send1[xq, :, i, part] = jnp.where(in_first_row, rows[2 * xq], rows[2 * xq + 1])

    pl.semaphore_wait(barrier, STRIPS - 1 + COLS - 1)

    for pz, px in plane():
        pltpu.make_async_remote_copy(
            src_ref=send1.at[px, pz], dst_ref=recv1.at[strip], send_sem=s1, recv_sem=r1,
            device_id=((pz << 2) + px, col), device_id_type=MESH,
        ).start()
    pltpu.make_async_copy(send1.at[x, z], recv1.at[strip], r1).start()

    m = 16 * x + 8 * core + z
    facet_of = upright(ints_v[0].astype(jnp.float32)).astype(jnp.int32)
    chosen = facet_of == lax.broadcasted_iota(jnp.int32, (SLOTS, SLOTS), 1)

    def by_slot(row):
        return jnp.sum(jnp.where(chosen, row.astype(jnp.float32), 0.0), axis=1, keepdims=True).astype(jnp.int32)

    ra, ca, vf, ve = (by_slot(ints_v[k]) for k in range(1, 5))
    block = (ra >> 6) + (m < (ra & 63)).astype(jnp.int32)
    facet_row = (m - ra) & 63
    row_weight = jnp.where((facet_row >= vf) & (facet_row < ve), squared_sine(facet_row, FH), 0.0)
    column_group = sum((ca >= FW * k).astype(jnp.int32) for k in range(1, COLS))
    first_class = ca - FW * column_group
    class_index = QUARTER * y + lax.broadcasted_iota(jnp.int32, (SLOTS, QUARTER), 1)
    upper = class_index >= first_class
    facet_col = class_index - first_class + jnp.where(upper, 0, FW)
    weight = row_weight * squared_sine(facet_col, FW)
    wide_lane = lax.broadcasted_iota(jnp.int32, (SLOTS, 2 * SLOTS), 1)
    wide_sub = lax.broadcasted_iota(jnp.int32, (SLOTS, 2 * SLOTS), 0)
    low_bin = (8 * block + column_group).astype(jnp.float32)
    bin_row = jnp.sum(jnp.where((wide_lane & 63) == wide_sub, low_bin, 0.0), axis=0, keepdims=True)
    bin_row = bin_row.astype(jnp.int32) + (wide_lane[:1] >> 6)
    one_hot = (wide_sub == bin_row).astype(jnp.float32).astype(jnp.bfloat16)
    scale = 1.0 / jnp.maximum(binned(one_hot, upper, weight), 0.5)

    wait_for(recv1, r1)
    stitched = binned(one_hot, upper, recv1[...].reshape(SLOTS, QUARTER)) * scale
    squares = stitched * stitched
    sums = squares[0:8]
    for q in range(1, 8):
        sums = sums + squares[8 * q : 8 * q + 8]
    psum[0] = sums[0:4]
    psum[1] = sums[4:8]
    tile[:, 0, :] = stitched

    place = 2 * x + core
    for dx in (2, 1, 3, 0):
        for dc in (1, 0):
            if dx or dc:
                px, pc = (x + dx) & 3, core ^ dc
                pltpu.make_async_remote_copy(
                    src_ref=psum.at[pc], dst_ref=pgot.at[place], send_sem=s3, recv_sem=r3,
                    device_id=((z << 2) + px, 2 * y + pc), device_id_type=MESH,
                ).start()
    pltpu.make_async_copy(psum.at[core], pgot.at[place], r3).start()

    row = 8 * core + z
    cols = pl.ds(pl.multiple_of(QUARTER * y, LANES), QUARTER)
    for dz in FAR_FIRST:
        for dg in (4, 3, 5, 2, 6, 1, 7, 0):
            if dz or dg:
                pz, pg = (z + dz) & 7, (col + dg) & 7
                pltpu.make_async_remote_copy(
                    src_ref=tile.at[(pz << 3) + pg], dst_ref=land.at[row, :, cols], send_sem=s2, recv_sem=r2,
                    device_id=((pz << 2) + x, pg), device_id_type=MESH,
                ).start()
    pltpu.make_async_copy(tile.at[(z << 3) + col], land.at[row, :, cols], r2).start()

    wait_for(pgot, r3)
    total = pgot[0]
    for k in range(1, 8):
        total = total + pgot[k]
    psend[:, 0, :] = total
    own_half = (col >> 2) == core
    for dz in FAR_FIRST:
        for k in range(4):
            def remote():
                pltpu.make_async_remote_copy(
                    src_ref=psend.at[k], dst_ref=pall.at[z, :, cols], send_sem=s4, recv_sem=r4,
                    device_id=((((z + dz) & 7) << 2) + x, 4 * core + k), device_id_type=MESH,
                ).start()

            if dz:
                remote()
            else:
                own = 4 * core + k == col
                pl.when(jnp.logical_not(own))(remote)

                @pl.when(own)
                def _():
                    pltpu.make_async_copy(psend.at[k], pall.at[z, :, cols], r4).start()

    wait_for(recv1.at[pl.ds(0, STRIPS - 1)], s1)
    wait_for(pgot.at[pl.ds(0, 7)], s3)
    wait_for(tile.at[pl.ds(0, 63)], s2)
    wait_for(tile.at[pl.ds(0, 31)], s4)

    @pl.when(jnp.logical_not(own_half))
    def _():
        wait_for(tile.at[0], s4)

    wait_for(land, r2)
    wait_for(pall, r4)


def finish(land, pall, out, power):
    for n in range(TILES):
        part = slice(LANES * n, LANES * (n + 1))
        out[:, part] = land[:, 0, part]
        power[n : n + 1, :] = jnp.sum(pall[:, 0, part], axis=0, keepdims=True) / (FH * 8)


def body(residuals, corr_rows, corr_cols, row_anchor, col_anchor, valid_first, valid_end, facet_of_slot):
    ints = (facet_of_slot, row_anchor, col_anchor, valid_first, valid_end)
    hbm = pl.BlockSpec(memory_space=pl.ANY)
    vmem = pl.BlockSpec(memory_space=pltpu.VMEM)
    f32, i32 = jnp.float32, jnp.int32
    dma = pltpu.SemaphoreType.DMA
    land, pall = pl.pallas_call(
        lambda a, b, c, *refs: kernel(a, b, c, refs[:5], refs[5:10], *refs[10:]),
        out_shape=(pltpu.VMEM((ROWS, 1, FW), f32), pltpu.VMEM((ZS, 1, FW), f32)),
        in_specs=[hbm] * 13,
        out_specs=(vmem, vmem),
        scratch_shapes=[
            pltpu.VMEM((2, FH, FW), f32),
            pltpu.VMEM((1, FH), f32),
            pltpu.VMEM((TILES, LANES), f32),
            pltpu.VMEM((5, 1, SLOTS), i32),
            pltpu.SMEM((5, SLOTS), i32),
            pltpu.VMEM((2, FH, LANES), f32),
            pltpu.VMEM((8, FW), f32),
            pltpu.VMEM((8, 8, QUARTER), f32),
            pltpu.VMEM((XS, ZS, 2, QUARTER), f32),
            pltpu.VMEM((STRIPS, 2, QUARTER), f32),
            pltpu.VMEM((64, 1, QUARTER), f32),
            pltpu.VMEM((2, 4, QUARTER), f32),
            pltpu.VMEM((8, 4, QUARTER), f32),
            pltpu.VMEM((4, 1, QUARTER), f32),
            dma((13,)),
        ]
        + [dma] * 8,
        compiler_params=pltpu.CompilerParams(collective_id=0, has_side_effects=True),
        name="restitch",
    )(
        residuals, corr_rows.reshape(1, FH), corr_cols.reshape(TILES, LANES),
        *(a.reshape(1, SLOTS) for a in ints), *ints,
    )
    stitched, power = pl.pallas_call(
        finish,
        out_shape=(jax.ShapeDtypeStruct((ROWS, FW), f32), jax.ShapeDtypeStruct((TILES, LANES), f32)),
        in_specs=[vmem, vmem],
        out_specs=(vmem, vmem),
        compiler_params=pltpu.CompilerParams(vmem_limit_bytes=4 << 20),
        name="finish",
    )(land, pall)
    return stitched, power.reshape(FW)


def solution(mesh):
    in_specs = (P("strip", None, None), P(), P(), P(), P(), P(), P(), P())
    out_specs = (P("strip", "col"), P("col"))
    return jax.shard_map(body, mesh=mesh, in_specs=in_specs, out_specs=out_specs, check_vma=False)
```
